256 devices in a mesh: grp: 64 (over z_lo, x, y), sub: 4 (over z_hi, core).
Axes of the slice: x: 4, y: 4, z: 8 (z_hi: 2, z_lo: 4; z = z_hi * 4 + z_lo), core: 2. Of those that a mesh axis runs over, the one named last changes fastest.
Arguments:
- blocks: bfloat16 [2048, 128, 128], P(('grp', 'sub')), may hold values from -0.5 to 0.5
- block_cols: int32 [2048], P(('grp', 'sub')), may hold values from 0 to 255, as said below
- far_slots: int32 [256, 256], P(('grp', 'sub')), may hold values from 0 to 7, as said below
- pair_lists: int32 [256, 4, 1024], P(('grp', 'sub')), may hold values from 0 to 7, as said below
Outputs:
- participation: float32 [32768], P(('grp', 'sub'))
- total: float32 [], replicated
The draws below stay inside these ranges and needn't reach their ends.
Inputs may be any that keep to these rules, and one draw needn't show every extreme that they name: `block_cols`: the block column of slot t is at most its block row t // 8. `far_slots`: the 4 slots of one block row and source group are distinct. `pair_lists`: rows 0 and 2 hold slot numbers below 8, row 1 positions below 4, row 3 holds 0 or 1; within one block row and source group no two triples share both their left slot and far position.
All inputs are finite; a program needn't handle non-finite values.
Results may differ from the reference program's by a relative error of at most 0.00035.
Values may be sent and summed in bfloat16 or wider, within the bound.
A program may use at most 64 MiB of HBM per device.

```python
import math
import jax
import jax.numpy as jnp
from jax import lax

BS = 128
KD = 8
FAR = 4
P_SIZE = 16
GROUPS = 64
ROWBLOCKS = 256
N_SUB = 4


def draw_block_cols(key, part):
    owners = jnp.arange(ROWBLOCKS * KD, dtype=jnp.int32) // KD
    first = jax.random.fold_in(key, 11)
    second = jax.random.fold_in(key, 12)
    diagonal = jax.random.randint(first, (ROWBLOCKS * KD,), 0, 3) == 0
    spread = jax.random.randint(second, (ROWBLOCKS * KD,), 0, owners + 1)
    return jnp.where(diagonal, owners, spread).astype(jnp.int32)


def build_lists(key):
    base = jax.random.fold_in(key, 30)
    width = GROUPS * P_SIZE
    scores = jax.random.randint(jax.random.fold_in(base, 1), (ROWBLOCKS, GROUPS, KD), 0, 2 ** 20) * KD
    scores = scores + jnp.arange(KD, dtype=jnp.int32)
    order = jnp.argsort(scores, axis=-1, stable=True).astype(jnp.int32)
    chosen_far = order[:, :, :FAR].reshape(ROWBLOCKS, GROUPS * FAR)
    pairs = FAR * KD
    pair_scores = jax.random.randint(jax.random.fold_in(base, 2), (ROWBLOCKS, GROUPS, pairs), 0, 2 ** 16) * pairs
    pair_scores = pair_scores + jnp.arange(pairs, dtype=jnp.int32)
    picked = jnp.argsort(pair_scores, axis=-1, stable=True).astype(jnp.int32)[:, :, :P_SIZE]
    left_slot = picked % KD
    far_place = picked // KD
    mask_slot = jax.random.randint(jax.random.fold_in(base, 3), (ROWBLOCKS, GROUPS, P_SIZE), 0, KD)
    triples = jnp.stack([left_slot, far_place, mask_slot], axis=1).reshape(ROWBLOCKS, 3, width)
    source = jnp.arange(width, dtype=jnp.int32) // P_SIZE
    bound = 4 * GROUPS - 3 * source
    draws = jax.random.randint(jax.random.fold_in(base, 4), (ROWBLOCKS, 1, width), 0, 4 * GROUPS)
    live = (draws < bound[None, None, :]).astype(jnp.int32)
    lists = jnp.concatenate([triples.astype(jnp.int32), live], axis=1)
    return (chosen_far.astype(jnp.int32), lists)


def draw_far_slots(key, part):
    return build_lists(key)[0]


def draw_pair_lists(key, part):
    return build_lists(key)[1]


def shard_levels(key, dims, split, least, top_value):
    gain = 1.0
    for axis_at, parts in split:
        steps = jax.random.uniform(jax.random.fold_in(jax.random.fold_in(key, 6), axis_at), (parts,), jnp.float32, least / len(split), top_value / len(split))
        gain = gain * jnp.repeat(jnp.exp(steps), dims[axis_at] // parts).reshape((-1,) + (1,) * (len(dims) - 1 - axis_at))
    return gain


def centred(key, dims, scale, most, pieces=(), held_as=jnp.bfloat16):
    entries = scale * jax.random.normal(key, dims, jnp.float32)
    if pieces:
        entries = entries * shard_levels(key, dims, pieces, -0.22, 0.18)
    return jnp.clip(entries, -most, most).astype(held_as)


def setup_inputs(seed: int = 0) -> dict:
    splits = jax.random.split(jax.random.key(seed), 5)
    blocks = centred(splits[0], (ROWBLOCKS * KD, BS, BS), 0.07, 0.5, ((0, 256),))
    block_cols = draw_block_cols(jax.random.fold_in(splits[4], 71), 0)
    far_slots = draw_far_slots(jax.random.fold_in(splits[4], 71), 0)
    pair_lists = draw_pair_lists(jax.random.fold_in(splits[4], 71), 0)
    return {"blocks": blocks, "block_cols": block_cols, "far_slots": far_slots, "pair_lists": pair_lists}


def reference(blocks, block_cols, far_slots, pair_lists):
    count = blocks.shape[0]
    size = blocks.shape[1]
    owners = jnp.arange(count, dtype=jnp.int32) // KD
    inner = jnp.arange(size, dtype=jnp.int32)
    strict = inner[:, None] > inner[None, :]
    on_diag = block_cols == owners
    masked = jnp.where(on_diag[:, None, None] & jnp.logical_not(strict)[None], 0.0, blocks.astype(jnp.float32))
    columns = jnp.arange(GROUPS * P_SIZE, dtype=jnp.int32)

    def one_row(row):
        lists = pair_lists[row]
        sub_index = row % N_SUB
        group_of = columns // P_SIZE
        source = group_of * N_SUB + sub_index
        far_slot = far_slots[row][group_of * FAR + lists[1]]
        left = masked[row * KD + lists[0]]
        far = masked[source * KD + far_slot]
        mask = masked[row * KD + lists[2]]
        product = jnp.einsum('wik,wkj->wij', left, far)
        sums = lax.optimization_barrier(jnp.sum(mask * product, axis=2))
        return lax.optimization_barrier(jnp.sum(lists[3].astype(jnp.float32)[:, None] * sums, axis=0))
    rows = lax.map(one_row, jnp.arange(ROWBLOCKS, dtype=jnp.int32))
    participation = rows.reshape(ROWBLOCKS * size)
    total = jnp.sum(participation) / math.sqrt(ROWBLOCKS * size)
    return (participation, total)
```

```python
import functools
import math

import jax
import jax.numpy as jnp
from jax import lax
from jax.experimental import pallas as pl
from jax.experimental.pallas import tpu as pltpu
from jax.sharding import Mesh
from jax.sharding import PartitionSpec as P

GRP = ("grp_0", "grp_1", "grp_2")
SUB = ("sub_0", "sub_1")
GRP_SUB = GRP + SUB
MESH_IDS = pl.DeviceIdType.MESH
R, D, L = 1, 2, 3


def kernel(
    blocks_hbm, cols_ref, far_hbm, lists_hbm,
    part_ref, total_ref,
    raw, own, r_near, r_far, q_near, q_zown, q_far,
    lists_v, far_v, lists_own, far_own, lists_near, far_near, lists_far, far_far,
    accum, part_send, part_recv, plane_recv, depth_send, depth_recv,
    load_sem, smem_sem,
    send_r, recv_r, send_q, recv_q, send_l, recv_l, send_f, recv_f,
    send_p, recv_p, send_t, recv_t, send_d, recv_d,
):
    z = lax.axis_index("grp_0")
    x = lax.axis_index("grp_1")
    y = lax.axis_index("grp_2")
    zh = lax.axis_index("sub_0")
    core = lax.axis_index("sub_1")
    kd, size = blocks_hbm.shape[0], blocks_hbm.shape[1]
    half = kd // 2
    other = 1 - core

    def at(dz, dx, dy):
        return (dz, lax.rem(x + dx, 4), lax.rem(y + dy, 4), zh, core)

    def row_at(dz, step):
        return at(dz, core * step, other * step)

    def src_at(dz, step):
        return at(dz, other * step, core * step)

    z1 = z + 1 - 2 * lax.rem(z, 2)
    z2 = lax.rem(z + 2, 4)
    place = x * 4 + y
    level = (zh * 4 + z) * 2 + core

    def plane_dev(p):
        return (z, p // 4, lax.rem(p, 4), zh, core)

    def level_dev(p):
        return (lax.rem(p // 2, 4), x, y, p // 8, lax.rem(p, 2))

    barrier = pltpu.get_barrier_semaphore()

    def greet(dev):
        pl.semaphore_signal(barrier, inc=1, device_id=dev, device_id_type=MESH_IDS)

    load = pltpu.make_async_copy(blocks_hbm, raw, load_sem.at[0])
    load.start()
    own_lists = pltpu.make_async_copy(lists_hbm, lists_own.at[0], load_sem.at[1])
    own_lists.start()
    own_far = pltpu.make_async_copy(far_hbm, far_own.at[0], load_sem.at[2])
    own_far.start()

    def greet_both(k, carry):
        greet(plane_dev(lax.rem(place + k, 16)))
        greet(level_dev(lax.rem(level + k, 16)))
        return carry

    lax.fori_loop(1, 16, greet_both, 0)
    for step in (R, D, L):
        greet(row_at(z1, step))

    zero = jnp.zeros((size, size), jnp.bfloat16)
    own[kd] = zero
    for s in range(3):
        r_near[s, kd] = zero
    for s in range(4):
        r_far[s, kd] = zero
    for s in range(8):
        accum[s] = jnp.zeros((size, size), jnp.float32)
    load.wait()
    me = ((z * 4 + x) * 4 + y) * 4 + zh * 2 + core
    rows = lax.broadcasted_iota(jnp.int32, (size, size), 0)
    cols = lax.broadcasted_iota(jnp.int32, (size, size), 1)
    for t in range(kd):
        shift = jnp.where(cols_ref[t] == me, 0, size)
        block = raw[t].astype(jnp.float32)
        own[t] = jnp.where(rows + shift > cols, block, 0.0).astype(jnp.bfloat16)

    pl.semaphore_wait(barrier, 33)

    def remote(src, dst, ssem, rsem, dev):
        return pltpu.make_async_remote_copy(
            src_ref=src, dst_ref=dst, send_sem=ssem, recv_sem=rsem,
            device_id=dev, device_id_type=MESH_IDS,
        )

    mine = own.at[pl.ds(0, kd)]
    first, second = pl.ds(0, half), pl.ds(half, half)
    whole = pl.ds(0, kd)

    def slot_r(o):
        return r_near.at[o - 1] if o < 4 else r_far.at[o - 4]

    def slot_q(o):
        if o < 4:
            return q_near.at[o - 1]
        return q_zown if o == 4 else q_far.at[o - 5]

    def ring_copies(slot, near, dev, base, ssem, rsem):
        zz = base
        return {
            "L": remote(near, slot(zz + L).at[whole], ssem.at[zz + 0], rsem.at[zz + 0], dev(z, 1)),
            "R": remote(near, slot(zz + R).at[whole], ssem.at[zz + 1], rsem.at[zz + 1], dev(z, 3)),
            "D1": remote(slot(zz + L).at[first], slot(zz + D).at[first], ssem.at[zz + 2], rsem.at[zz + 2], dev(z, 1)),
            "D2": remote(slot(zz + R).at[second], slot(zz + D).at[second], ssem.at[zz + 3], rsem.at[zz + 3], dev(z, 3)),
        }

    rn = ring_copies(slot_r, mine, row_at, 0, send_r, recv_r)
    qn = ring_copies(slot_q, mine, src_at, 0, send_q, recv_q)
    rf = ring_copies(slot_r, slot_r(4).at[whole], row_at, 4, send_r, recv_r)
    qf = ring_copies(slot_q, slot_q(4).at[whole], src_at, 4, send_q, recv_q)
    rz = remote(mine, slot_r(4).at[whole], send_r.at[8], recv_r.at[8], row_at(z1, 0))
    qz = remote(mine, slot_q(4).at[whole], send_q.at[8], recv_q.at[8], src_at(z2, 0))

    for copy in (rz, rn["L"], rn["R"], qn["L"], qn["R"], qz):
        copy.start()

    back = {0: 0, R: L, D: D, L: R}
    list_copies = []
    for o in range(1, 8):
        dev = row_at(z if o < 4 else z1, o % 4)
        there = (o // 4) * 4 + back[o % 4]
        list_copies.append(remote(lists_hbm, lists_v.at[there], send_l.at[o], recv_l.at[there], dev))
        list_copies.append(remote(far_hbm, far_v.at[there], send_f.at[o], recv_f.at[there], dev))
    for copy in list_copies:
        copy.start()
    own_lists.wait()
    own_far.wait()

    ub = x + core * (y - x)
    ua = y + core * (x - y)

    def source_group(o):
        b = lax.rem(ub + o, 4)
        zq = z if o < 4 else z2
        xq = b + core * (ua - b)
        yq = ua + core * (b - ua)
        return zq * 16 + xq * 4 + yq

    def triples(row_ref, lists, fars, rr, q_ref, q_index, group, acc):
        base = group * 16

        def pick(w):
            left = lists[rr, 0, base + w]
            far = fars[rr, 0, group * 4 + lists[rr, 1, base + w]]
            mask = lists[rr, 2, base + w]
            left = jnp.where(lists[rr, 3, base + w] > 0, left, kd)
            far_block = q_ref[far] if q_index is None else q_ref[q_index, far]
            if row_ref is own:
                return own[left], far_block, own[mask]
            return row_ref[rr, left], far_block, row_ref[rr, mask]

        for w in range(0, 16, 2):
            l0, f0, m0 = pick(w)
            l1, f1, m1 = pick(w + 1)
            lhs = jnp.concatenate([l0, l1], axis=1)
            rhs = jnp.concatenate(
                [jnp.concatenate([f0, zero], axis=1), jnp.concatenate([zero, f1], axis=1)], axis=0
            )
            product = jnp.dot(lhs, rhs, preferred_element_type=jnp.float32)
            acc = acc + product[:, :size] * m0.astype(jnp.float32)
            acc = acc + product[:, size:] * m1.astype(jnp.float32)
        return acc

    row_groups = {
        "O": (own, lists_own, far_own, 0, 1),
        "N": (r_near, lists_near, far_near, 1, 3),
        "F": (r_far, lists_far, far_far, 4, 4),
    }
    src_groups = {
        "O": [(own, None, 0)],
        "N": [(q_near, o - 1, o) for o in (R, D, L)],
        "Z": [(q_zown, None, 4)],
        "F": [(q_far, o - 1, 4 + o) for o in (R, D, L)],
    }

    def work(rg, qgs):
        row_ref, lists, fars, slot0, count = row_groups[rg]

        def one(rr, carry):
            acc = accum[slot0 + rr]
            for qg in qgs:
                for q_ref, q_index, o in src_groups[qg]:
                    acc = triples(row_ref, lists, fars, rr, q_ref, q_index, source_group(o), acc)
            accum[slot0 + rr] = acc
            return carry

        if count == 1:
            one(0, 0)
        else:
            lax.fori_loop(0, count, one, 0)

    def forward(ring):
        ring["L"].wait_recv()
        ring["D1"].start()
        ring["R"].wait_recv()
        ring["D2"].start()

    work("O", ["O"])
    forward(rn)
    forward(qn)
    rz.wait_recv()
    rf["L"].start()
    rf["R"].start()

    moves = []
    for o in range(1, 8):
        dst_l = lists_near.at[o - 1] if o < 4 else lists_far.at[o - 4]
        dst_f = far_near.at[o - 1] if o < 4 else far_far.at[o - 4]
        remote(lists_hbm, lists_v.at[o], send_l.at[o], recv_l.at[o], row_at(z1, 0)).wait_recv()
        remote(far_hbm, far_v.at[o], send_f.at[o], recv_f.at[o], row_at(z1, 0)).wait_recv()
        moves.append(pltpu.make_async_copy(lists_v.at[o], dst_l, smem_sem.at[o]))
        moves.append(pltpu.make_async_copy(far_v.at[o], dst_f, smem_sem.at[8 + o]))
    for move in moves:
        move.start()
    for move in moves:
        move.wait()

    qz.wait_recv()
    qf["L"].start()
    qf["R"].start()
    forward(rf)
    for ring in (rn, qn):
        ring["D1"].wait_recv()
        ring["D2"].wait_recv()
    work("O", ["N", "Z"])
    work("N", ["O", "N", "Z"])
    forward(qf)
    rf["D1"].wait_recv()
    rf["D2"].wait_recv()
    work("F", ["O", "N", "Z"])
    qf["D1"].wait_recv()
    qf["D2"].wait_recv()
    for rg in ("O", "N", "F"):
        work(rg, ["F"])

    def row_of(s):
        return jnp.sum(jnp.transpose(accum[s]), axis=0, keepdims=True)

    whole_sum = row_of(0)
    part_recv[0] = whole_sum
    for o in range(1, 8):
        row = row_of(o)
        part_send[o] = row
        whole_sum = whole_sum + row
    plane_recv[place] = whole_sum
    part_send[0] = whole_sum

    def plane_copy(p):
        return remote(part_send.at[0], plane_recv.at[place], send_t.at[p], recv_t.at[place], plane_dev(p))

    def level_copy(p):
        return remote(depth_send, depth_recv.at[level], send_d.at[p], recv_d.at[level], level_dev(p))

    def plane_start(k, carry):
        plane_copy(lax.rem(place + k, 16)).start()
        return carry

    lax.fori_loop(1, 16, plane_start, 0)
    part_copies = []
    for o in range(1, 8):
        dev = row_at(z if o < 4 else z1, o % 4)
        there = (o // 4) * 4 + back[o % 4]
        part_copies.append(remote(part_send.at[o], part_recv.at[there], send_p.at[o], recv_p.at[there], dev))
    for copy in part_copies:
        copy.start()

    def plane_wait(k, carry):
        p = lax.rem(place + k, 16)
        remote(part_send.at[0], plane_recv.at[p], send_t.at[p], recv_t.at[p], plane_dev(p)).wait_recv()
        return carry

    lax.fori_loop(1, 16, plane_wait, 0)
    depth_sum = plane_recv[0]
    for p in range(1, 16):
        depth_sum = depth_sum + plane_recv[p]
    depth_send[...] = depth_sum
    depth_recv[level] = depth_sum

    def level_start(k, carry):
        level_copy(lax.rem(level + k, 16)).start()
        return carry

    lax.fori_loop(1, 16, level_start, 0)

    for o in range(1, 8):
        remote(part_send.at[o], part_recv.at[o], send_p.at[o], recv_p.at[o], row_at(z1, 0)).wait_recv()
    participation = part_recv[0]
    for o in range(1, 8):
        participation = participation + part_recv[o]
    part_ref[...] = participation

    def level_wait(k, carry):
        p = lax.rem(level + k, 16)
        remote(depth_send, depth_recv.at[p], send_d.at[p], recv_d.at[p], level_dev(p)).wait_recv()
        return carry

    lax.fori_loop(1, 16, level_wait, 0)
    grand = depth_recv[0]
    for p in range(1, 16):
        grand = grand + depth_recv[p]
    total_ref[...] = jnp.sum(grand, axis=1, keepdims=True) * (1.0 / math.sqrt(256 * size))

    for ring in (rn, qn, rf, qf):
        for copy in ring.values():
            copy.wait_send()
    rz.wait_send()
    qz.wait_send()
    for copy in list_copies + part_copies:
        copy.wait_send()

    def sent(k, carry):
        plane_copy(lax.rem(place + k, 16)).wait_send()
        level_copy(lax.rem(level + k, 16)).wait_send()
        return carry

    lax.fori_loop(1, 16, sent, 0)


def local(blocks, block_cols, far_slots, pair_lists):
    kd, size = blocks.shape[0], blocks.shape[1]
    lists = pair_lists[0]
    width = lists.shape[1]
    fars = far_slots.shape[1]
    block = (size, size)
    dma = pltpu.SemaphoreType.DMA
    smem = pltpu.SMEM
    vmem = pltpu.VMEM
    bf16, f32, i32 = jnp.bfloat16, jnp.float32, jnp.int32
    participation, total = pl.pallas_call(
        kernel,
        out_shape=(
            jax.ShapeDtypeStruct((1, size), f32),
            jax.ShapeDtypeStruct((1, 1), f32),
        ),
        in_specs=[
            pl.BlockSpec(memory_space=pl.ANY),
            pl.BlockSpec(memory_space=pltpu.SMEM),
            pl.BlockSpec(memory_space=pl.ANY),
            pl.BlockSpec(memory_space=pl.ANY),
        ],
        out_specs=(
            pl.BlockSpec(memory_space=pltpu.VMEM),
            pl.BlockSpec(memory_space=pltpu.VMEM),
        ),
        scratch_shapes=[
            vmem((kd,) + block, bf16),
            vmem((kd + 1,) + block, bf16),
            vmem((3, kd + 1) + block, bf16),
            vmem((4, kd + 1) + block, bf16),
            vmem((3, kd) + block, bf16),
            vmem((kd,) + block, bf16),
            vmem((3, kd) + block, bf16),
            vmem((8, 4, width), i32),
            vmem((8, 1, fars), i32),
            smem((1, 4, width), i32),
            smem((1, 1, fars), i32),
            smem((3, 4, width), i32),
            smem((3, 1, fars), i32),
            smem((4, 4, width), i32),
            smem((4, 1, fars), i32),
            vmem((8,) + block, f32),
            vmem((8, 1, size), f32),
            vmem((8, 1, size), f32),
            vmem((16, 1, size), f32),
            vmem((1, size), f32),
            vmem((16, 1, size), f32),
            dma((3,)),
            dma((16,)),
            dma((9,)), dma((9,)), dma((9,)), dma((9,)),
            dma((8,)), dma((8,)), dma((8,)), dma((8,)),
            dma((8,)), dma((8,)), dma((16,)), dma((16,)), dma((16,)), dma((16,)),
        ],
        compiler_params=pltpu.CompilerParams(
            collective_id=0, has_side_effects=True, vmem_limit_bytes=48 * 1024 * 1024
        ),
    )(blocks, block_cols, far_slots[:, None, :][0], pair_lists[0])
    return (participation.reshape(size), total.reshape(()))


def solution(mesh):
    torus = Mesh(mesh.devices.reshape(4, 4, 4, 2, 2), GRP_SUB)
    in_specs = (P(GRP_SUB, None, None), P(GRP_SUB), P(GRP_SUB, None), P(GRP_SUB, None, None))
    out_specs = (P(GRP_SUB), P())
    return jax.shard_map(local, mesh=torus, in_specs=in_specs, out_specs=out_specs, check_vma=False)
```

```python
import functools
import math

import jax
import jax.numpy as jnp
from jax import lax
from jax.experimental import pallas as pl
from jax.experimental.pallas import tpu as pltpu
from jax.sharding import Mesh
from jax.sharding import PartitionSpec as P

GRP = ("grp_0", "grp_1", "grp_2")
SUB = ("sub_0", "sub_1")
GRP_SUB = GRP + SUB
MESH_IDS = pl.DeviceIdType.MESH
R, D, L = 1, 2, 3


def kernel(
    blocks_hbm, cols_hbm, far_hbm, lists_hbm,
    part_ref,
    raw, own, r_nlr, r_nd, r_zo, r_zlr, r_zd, q_nlr, q_nd, q_zo, q_zlr, q_zd,
    lists_v, far_v, lists_own, far_own, lists_near, far_near, lists_far, far_far, cols_s,
    accum, part_send, part_recv, plane_recv, depth_send, depth_recv,
    load_sem, smem_sem,
    send_r, recv_r, send_q, recv_q, send_l, recv_l, send_m, recv_m, send_f, recv_f,
    send_p, recv_p, send_t, recv_t, send_d, recv_d, tokens,
):
    z = lax.axis_index("grp_0")
    x = lax.axis_index("grp_1")
    y = lax.axis_index("grp_2")
    zh = lax.axis_index("sub_0")
    core = lax.axis_index("sub_1")
    kd, size = blocks_hbm.shape[0], blocks_hbm.shape[1]
    half, quarter = kd // 2, kd // 4
    oc, oh = 1 - core, 1 - zh
    z1 = z + 1 - 2 * lax.rem(z, 2)
    z2 = lax.rem(z + 2, 4)
    z3 = 3 - z
    xs = [x] + [lax.rem(x + o, 4) for o in (1, 2, 3)]
    ys = [y] + [lax.rem(y + o, 4) for o in (1, 2, 3)]
    back = (0, L, D, R)

    def row_at(zz, o):
        return (zz, x + core * (xs[o] - x), y + oc * (ys[o] - y), zh, core)

    def src_at(zz, o):
        return (zz, x + oc * (xs[o] - x), y + core * (ys[o] - y), zh, core)

    plane = [(dx, dy) for dx in range(4) for dy in range(4)][1:]
    depth = [(t, c, h) for t in range(4) for c in range(2) for h in range(2)][1:]
    place = x * 4 + y
    level = (zh * 4 + z) * 2 + core

    def plane_dev(k):
        dx, dy = plane[k]
        return (z, xs[dx], ys[dy], zh, core)

    def level_dev(k):
        t, c, h = depth[k]
        return ((z, z1, z2, z3)[t], x, y, (zh, oh)[h], (core, oc)[c])

    def local_copy(src, dst, sem):
        return pltpu.make_async_copy(src, dst, sem)

    def remote(src, dst, ssem, rsem, dev):
        return pltpu.make_async_remote_copy(
            src_ref=src, dst_ref=dst, send_sem=ssem, recv_sem=rsem,
            device_id=dev, device_id_type=MESH_IDS,
        )

    def columns(zz):
        return pl.ds(pl.multiple_of(zz * 256, 256), 256)

    barrier = pltpu.get_barrier_semaphore()
    load = local_copy(blocks_hbm, raw, load_sem.at[0])
    load.start()
    load_cols = local_copy(cols_hbm, cols_s, load_sem.at[1])
    load_cols.start()
    greeted = [row_at(z, o) for o in (R, D, L)] + [src_at(z, o) for o in (R, D, L)]
    greeted += [row_at(z1, o) for o in range(4)] + [src_at(z2, 0)]
    odd = lax.rem(z, 2)
    turned = lax.rem(z + 2 * odd + 3, 4)
    crossed = odd * (z // 3) + (1 - odd) * (1 - (z + 3) // 4)
    beyond = (turned, x, y, zh + crossed * (oh - zh), core)
    greeted += [(z, x, y, zh, oc), beyond]
    for dev in greeted:
        pl.semaphore_signal(barrier, inc=1, device_id=dev, device_id_type=MESH_IDS)
    own_moves = [
        local_copy(lists_hbm.at[:, columns(z)], lists_own.at[0, 0], load_sem.at[2]),
        local_copy(lists_hbm.at[:, columns(z2)], lists_own.at[0, 1], load_sem.at[3]),
        local_copy(far_hbm, far_own.at[0], load_sem.at[4]),
    ]
    for move in own_moves:
        move.start()

    zero = jnp.zeros((size, size), jnp.bfloat16)
    for ref, count in ((own, 0), (r_nlr, 2), (r_nd, 1), (r_zo, 1), (r_zlr, 2), (r_zd, 1)):
        for s in range(max(count, 1)):
            if count:
                ref[s, kd] = zero
            else:
                ref[kd] = zero
    for s in range(8):
        accum[s] = jnp.zeros((size, size), jnp.float32)
    load_cols.wait()
    load.wait()
    me = ((z * 4 + x) * 4 + y) * 4 + zh * 2 + core
    rows = lax.broadcasted_iota(jnp.int32, (size, size), 0)
    cols = lax.broadcasted_iota(jnp.int32, (size, size), 1)
    for t in range(kd):
        shift = jnp.where(cols_s[t] == me, 0, size)
        block = raw[t].astype(jnp.float32)
        own[t] = jnp.where(rows + shift > cols, block, 0.0).astype(jnp.bfloat16)

    pl.semaphore_wait(barrier, len(greeted))

    def token(k):
        for dev in (row_at(z1, 0), beyond):
            pl.semaphore_signal(tokens.at[k], inc=1, device_id=dev, device_id_type=MESH_IDS)

    def await_token(k):
        pl.semaphore_wait(tokens.at[k], 2)

    token(0)

    h1, h2 = pl.ds(0, half), pl.ds(half, half)

    def slot_r(o):
        return {R: r_nlr.at[0], L: r_nlr.at[1], D: r_nd.at[0], 4: r_zo.at[0],
                4 + R: r_zlr.at[0], 4 + L: r_zlr.at[1], 4 + D: r_zd.at[0]}[o]

    def slot_q(o):
        return {R: q_nlr.at[0], L: q_nlr.at[1], D: q_nd.at[0], 4: q_zo.at[0],
                4 + R: q_zlr.at[0], 4 + L: q_zlr.at[1], 4 + D: q_zd.at[0]}[o]

    def ring_copies(slot, src, dev, base, ssem, rsem, first_sem, parts, passed):
        right, left = dev(z, 1), dev(z, 3)
        ring, k = {}, first_sem
        for name, o, to in (("L", L, right), ("R", R, left)):
            for p, part in enumerate(parts):
                ring[name + str(p)] = remote(src.at[part], slot(base + o).at[part], ssem.at[k], rsem.at[k], to)
                k += 1
        for p, part in enumerate(parts):
            o, to = (L, right) if passed[p] in "Ll" else (R, left)
            via, to = (slot(base + o), to) if passed[p] in "LR" else (src, dev(z, D))
            ring["D" + str(p)] = remote(via.at[part], slot(base + D).at[part], ssem.at[k], rsem.at[k], to)
            k += 1
        return ring

    halves = (h1, h2)
    quarters = tuple(pl.ds(p * quarter, quarter) for p in range(4))
    rn = ring_copies(slot_r, own, row_at, 0, send_r, recv_r, 0, halves, "LR")
    qn = ring_copies(slot_q, own, src_at, 0, send_q, recv_q, 0, halves, "LR")
    rf = ring_copies(slot_r, slot_r(4), row_at, 4, send_r, recv_r, 6, quarters, "LRlr")
    qf = ring_copies(slot_q, slot_q(4), src_at, 4, send_q, recv_q, 6, quarters, "LRlr")
    rz = [remote(own.at[h], slot_r(4).at[h], send_r.at[18 + k], recv_r.at[18 + k], row_at(z1, 0)) for k, h in enumerate(quarters)]
    qz = [remote(own.at[h], slot_q(4).at[h], send_q.at[18 + k], recv_q.at[18 + k], src_at(z2, 0)) for k, h in enumerate(quarters)]

    for copy in rz + qz:
        copy.start()
    for ring in (rn, qn):
        ring["L0"].start()
        ring["R1"].start()
    for ring in (rn, qn):
        ring["L1"].start()
        ring["R0"].start()

    list_copies = []
    for o in range(1, 8):
        zz, zt = (z, z2) if o < 4 else (z1, z3)
        dev = row_at(zz, o % 4)
        there = (o // 4) * 4 + back[o % 4]
        list_copies.append(remote(lists_hbm.at[:, columns(zz)], lists_v.at[there, 0], send_l.at[o], recv_l.at[there], dev))
        list_copies.append(remote(lists_hbm.at[:, columns(zt)], lists_v.at[there, 1], send_m.at[o], recv_m.at[there], dev))
        list_copies.append(remote(far_hbm, far_v.at[there], send_f.at[o], recv_f.at[there], dev))
    for copy in list_copies:
        copy.start()

    ub = x + core * (y - x)
    ua = y + core * (x - y)

    def source_place(o):
        b = lax.rem(ub + o, 4)
        xq = b + core * (ua - b)
        yq = ua + core * (b - ua)
        return xq * 4 + yq

    def triples(row_ref, lists, fars, rr, o, acc):
        at_place = source_place(o % 4)
        base = at_place * 16
        far_base = (z if o < 4 else z2) * 64 + at_place * 4
        t = o // 4

        def pick(w):
            left = lists[rr, t, 0, base + w]
            far = fars[rr, 0, far_base + lists[rr, t, 1, base + w]]
            mask = lists[rr, t, 2, base + w]
            left = jnp.where(lists[rr, t, 3, base + w] > 0, left, kd)
            q_ref, q_index = {
                0: (own, None), R: (q_nlr, 0), L: (q_nlr, 1), D: (q_nd, 0), 4: (q_zo, 0),
                4 + R: (q_zlr, 0), 4 + L: (q_zlr, 1), 4 + D: (q_zd, 0),
            }[o]
            far_block = q_ref[far] if q_index is None else q_ref[q_index, far]
            if row_ref is own:
                return own[left], far_block, own[mask]
            at_row = 0 if row_ref is not r_nlr and row_ref is not r_zlr else rr_local
            return row_ref[at_row, left], far_block, row_ref[at_row, mask]

        rr_local = row_local[0]
        for w in range(0, 16, 2):
            l0, f0, m0 = pick(w)
            l1, f1, m1 = pick(w + 1)
            lhs = jnp.concatenate([l0, l1], axis=1)
            rhs = jnp.concatenate(
                [jnp.concatenate([f0, zero], axis=1), jnp.concatenate([zero, f1], axis=1)], axis=0
            )
            product = jnp.dot(lhs, rhs, preferred_element_type=jnp.float32)
            acc = acc + product[:, :size] * m0.astype(jnp.float32)
            acc = acc + product[:, size:] * m1.astype(jnp.float32)
        return acc

    row_local = [0]
    row_groups = {
        "O": (own, lists_own, far_own, (0,), (0,)),
        "LR": (r_nlr, lists_near, far_near, (R, L), (0, 2)),
        "D": (r_nd, lists_near, far_near, (D,), (1,)),
        "zO": (r_zo, lists_far, far_far, (4,), (0,)),
        "zLR": (r_zlr, lists_far, far_far, (4 + R, 4 + L), (1, 3)),
        "zD": (r_zd, lists_far, far_far, (4 + D,), (2,)),
    }
    sources = {"O": (0,), "LR": (R, L), "D": (D,), "zO": (4,), "zLR": (4 + R, 4 + L), "zD": (4 + D,)}

    def work(rgs, qgs):
        for rg in rgs:
            row_ref, lists, fars, slots, at_list = row_groups[rg]

            def one(k, carry):
                row_local[0] = k
                slot = slots[0] if len(slots) == 1 else slots[0] + 2 * k
                rr = at_list[0] if len(slots) == 1 else at_list[0] + 2 * k
                acc = accum[slot]
                for qg in qgs:
                    for o in sources[qg]:
                        acc = triples(row_ref, lists, fars, rr, o, acc)
                accum[slot] = acc
                return carry

            if len(slots) == 1:
                one(0, 0)
            else:
                for k in range(len(slots)):
                    one(k, 0)

    def list_moves(slots):
        moves = []
        for o in slots:
            k, dst_l, dst_f = (o - 1, lists_near, far_near) if o < 4 else (o - 4, lists_far, far_far)
            dev = row_at(z1, 0)
            remote(lists_hbm.at[:, columns(z)], lists_v.at[o, 0], send_l.at[o], recv_l.at[o], dev).wait_recv()
            remote(lists_hbm.at[:, columns(z)], lists_v.at[o, 1], send_m.at[o], recv_m.at[o], dev).wait_recv()
            remote(far_hbm, far_v.at[o], send_f.at[o], recv_f.at[o], dev).wait_recv()
            moves.append(local_copy(lists_v.at[o], dst_l.at[k], smem_sem.at[o]))
            moves.append(local_copy(far_v.at[o], dst_f.at[k], smem_sem.at[8 + o]))
        for move in moves:
            move.start()
        return moves

    def finish(moves):
        for move in moves:
            move.wait()

    def got(ring, *names):
        for name in names:
            ring[name].wait_recv()

    def spread(zcopies, ring, *parts):
        for p in parts:
            zcopies[p].wait_recv()
            if p > 1:
                ring["D" + str(p)].start()
            ring["L" + str(p)].start()
            ring["R" + str(p)].start()

    def relay(ring, *names):
        for name in names:
            ring[name].wait_recv()
            ring["D" + name[1]].start()

    finish(own_moves)
    work(["O"], ["O"])
    await_token(0)
    token(1)
    relay(rn, "L0", "R1")
    relay(qn, "L0", "R1")
    spread(rz, rf, 0, 1)
    await_token(1)
    token(2)
    got(rn, "L1", "R0")
    got(qn, "L1", "R0")
    finish(list_moves((1, 2, 3)))
    work(["O"], ["LR"])
    spread(rz, rf, 2, 3)
    spread(qz, qf, 0)
    work(["LR"], ["O", "LR"])
    relay(rf, "L0", "R1")
    spread(qz, qf, 1)
    got(rn, "D0", "D1")
    got(qn, "D0", "D1")
    work(["O", "LR"], ["D"])
    spread(qz, qf, 2)
    work(["D"], ["O", "LR", "D"])
    relay(qf, "L0", "R1")
    await_token(2)
    finish(list_moves((4, 5, 6, 7)))
    work(["zO"], ["O", "LR", "D"])
    spread(qz, qf, 3)
    got(rf, "R0", "L1", "L2", "R2", "L3", "R3")
    work(["zLR"], ["O", "LR", "D"])
    work(["O", "LR", "D", "zO", "zLR"], ["zO"])
    got(rf, "D0", "D1", "D2", "D3")
    work(["zD"], ["O", "LR", "D", "zO"])
    got(qf, "R0", "L1", "L2", "R2", "L3", "R3")
    work(["O", "LR", "D", "zO", "zLR", "zD"], ["zLR"])
    got(qf, "D0", "D1", "D2", "D3")
    work(["O", "LR", "D", "zO", "zLR", "zD"], ["zD"])

    def row_of(s):
        return jnp.sum(jnp.transpose(accum[s]), axis=0, keepdims=True)

    partials = [row_of(s) for s in range(8)]
    whole_sum = partials[0]
    for s in range(1, 8):
        part_send[s] = partials[s]
        whole_sum = whole_sum + partials[s]
    part_send[0] = whole_sum
    plane_recv[place] = whole_sum
    part_recv[0] = partials[0]

    def plane_there(k):
        dx, dy = plane[k]
        return plane.index(((4 - dx) % 4, (4 - dy) % 4))

    plane_copies = [
        remote(part_send.at[0], plane_recv.at[place], send_t.at[k], recv_t.at[plane_there(k)], plane_dev(k))
        for k in range(15)
    ]
    for copy in plane_copies:
        copy.start()
    part_copies = []
    for o in range(1, 8):
        dev = row_at(z if o < 4 else z1, o % 4)
        there = (o // 4) * 4 + back[o % 4]
        part_copies.append(remote(part_send.at[o], part_recv.at[there], send_p.at[o], recv_p.at[there], dev))
    for copy in part_copies:
        copy.start()

    for o in range(1, 8):
        remote(part_send.at[o], part_recv.at[o], send_p.at[o], recv_p.at[o], row_at(z1, 0)).wait_recv()
    for k in range(15):
        remote(part_send.at[0], plane_recv.at[place], send_t.at[k], recv_t.at[k], plane_dev(k)).wait_recv()
    depth_sum = plane_recv[0]
    for p in range(1, 16):
        depth_sum = depth_sum + plane_recv[p]
    depth_send[...] = depth_sum
    depth_recv[level] = depth_sum
    level_copies = [
        remote(depth_send, depth_recv.at[level], send_d.at[k], recv_d.at[k], level_dev(k)) for k in range(15)
    ]
    for copy in level_copies:
        copy.start()
    participation = part_recv[0]
    for o in range(1, 8):
        participation = participation + part_recv[o]
    part_ref[0:1] = participation

    for ring in (rn, qn, rf, qf):
        for copy in ring.values():
            copy.wait_send()
    for copy in rz + qz + list_copies + part_copies + plane_copies:
        copy.wait_send()
    for copy in level_copies:
        copy.wait_recv()
    grand = depth_recv[0]
    for p in range(1, 16):
        grand = grand + depth_recv[p]
    part_ref[1:2] = jnp.broadcast_to(jnp.sum(grand, axis=1, keepdims=True) * (1.0 / math.sqrt(256 * size)), (1, size))
    for copy in level_copies:
        copy.wait_send()


def local(blocks, block_cols, far_slots, pair_lists):
    kd, size = blocks.shape[0], blocks.shape[1]
    fars = far_slots.shape[1]
    block = (size, size)
    dma = pltpu.SemaphoreType.DMA
    smem = pltpu.SMEM
    vmem = pltpu.VMEM
    bf16, f32, i32 = jnp.bfloat16, jnp.float32, jnp.int32
    result = pl.pallas_call(
        kernel,
        out_shape=jax.ShapeDtypeStruct((2, size), f32),
        in_specs=[pl.BlockSpec(memory_space=pl.ANY)] * 4,
        out_specs=pl.BlockSpec(memory_space=pltpu.VMEM),
        scratch_shapes=[
            vmem((kd,) + block, bf16),
            vmem((kd + 1,) + block, bf16),
            vmem((2, kd + 1) + block, bf16),
            vmem((1, kd + 1) + block, bf16),
            vmem((1, kd + 1) + block, bf16),
            vmem((2, kd + 1) + block, bf16),
            vmem((1, kd + 1) + block, bf16),
            vmem((2, kd) + block, bf16),
            vmem((1, kd) + block, bf16),
            vmem((1, kd) + block, bf16),
            vmem((2, kd) + block, bf16),
            vmem((1, kd) + block, bf16),
            vmem((8, 2, 4, 256), i32),
            vmem((8, 1, fars), i32),
            smem((1, 2, 4, 256), i32),
            smem((1, 1, fars), i32),
            smem((3, 2, 4, 256), i32),
            smem((3, 1, fars), i32),
            smem((4, 2, 4, 256), i32),
            smem((4, 1, fars), i32),
            smem((kd,), i32),
            vmem((8,) + block, f32),
            vmem((8, 1, size), f32),
            vmem((8, 1, size), f32),
            vmem((16, 1, size), f32),
            vmem((1, size), f32),
            vmem((16, 1, size), f32),
            dma((5,)),
            dma((16,)),
            dma((22,)), dma((22,)), dma((22,)), dma((22,)),
            dma((8,)), dma((8,)), dma((8,)), dma((8,)), dma((8,)), dma((8,)),
            dma((8,)), dma((8,)), dma((15,)), dma((15,)), dma((15,)), dma((15,)),
            pltpu.SemaphoreType.REGULAR((3,)),
        ],
        compiler_params=pltpu.CompilerParams(
            collective_id=0, has_side_effects=True, vmem_limit_bytes=60 * 1024 * 1024
        ),
    )(blocks, block_cols, far_slots, pair_lists[0])
    return (result[0], result[1, 0])


def solution(mesh):
    torus = Mesh(mesh.devices.reshape(4, 4, 4, 2, 2), GRP_SUB)
    in_specs = (P(GRP_SUB, None, None), P(GRP_SUB), P(GRP_SUB, None), P(GRP_SUB, None, None))
    out_specs = (P(GRP_SUB), P())
    return jax.shard_map(local, mesh=torus, in_specs=in_specs, out_specs=out_specs, check_vma=False)
```

```python
import functools
import math

import jax
import jax.numpy as jnp
from jax import lax
from jax.experimental import pallas as pl
from jax.experimental.pallas import tpu as pltpu
from jax.sharding import Mesh
from jax.sharding import PartitionSpec as P

GRP = ("grp_0", "grp_1", "grp_2")
SUB = ("sub_0", "sub_1")
GRP_SUB = GRP + SUB
MESH_IDS = pl.DeviceIdType.MESH
R, D, L = 1, 2, 3


def kernel(
    blocks_hbm, cols_hbm, far_hbm, lists_hbm,
    part_ref,
    raw, own, r_nlr, r_nd, r_zo, r_zlr, r_zd, q_nlr, q_nd, q_zo, q_zlr, q_zd,
    lists_v, far_v, lists_own, far_own, lists_near, far_near, lists_far, far_far, cols_s,
    accum, part_send, part_recv, plane_recv, depth_send, depth_recv,
    load_sem, smem_sem,
    send_r, recv_r, send_q, recv_q, send_l, recv_l, send_m, recv_m, send_f, recv_f,
    send_p, recv_p, send_t, recv_t, send_d, recv_d, tokens,
):
    z = lax.axis_index("grp_0")
    x = lax.axis_index("grp_1")
    y = lax.axis_index("grp_2")
    zh = lax.axis_index("sub_0")
    core = lax.axis_index("sub_1")
    kd, size = blocks_hbm.shape[0], blocks_hbm.shape[1]
    half, quarter = kd // 2, kd // 4
    oc, oh = 1 - core, 1 - zh
    z1 = z + 1 - 2 * lax.rem(z, 2)
    z2 = lax.rem(z + 2, 4)
    z3 = 3 - z
    xs = [x] + [lax.rem(x + o, 4) for o in (1, 2, 3)]
    ys = [y] + [lax.rem(y + o, 4) for o in (1, 2, 3)]
    back = (0, L, D, R)

    def row_at(zz, o):
        return (zz, x + core * (xs[o] - x), y + oc * (ys[o] - y), zh, core)

    def src_at(zz, o):
        return (zz, x + oc * (xs[o] - x), y + core * (ys[o] - y), zh, core)

    plane = [(dx, dy) for dx in range(4) for dy in range(4)][1:]
    depth = [(t, c, h) for t in range(4) for c in range(2) for h in range(2)][1:]
    place = x * 4 + y
    level = (zh * 4 + z) * 2 + core

    def plane_dev(k):
        dx, dy = plane[k]
        return (z, xs[dx], ys[dy], zh, core)

    def level_dev(k):
        t, c, h = depth[k]
        return ((z, z1, z2, z3)[t], x, y, (zh, oh)[h], (core, oc)[c])

    def local_copy(src, dst, sem):
        return pltpu.make_async_copy(src, dst, sem)

    def remote(src, dst, ssem, rsem, dev):
        return pltpu.make_async_remote_copy(
            src_ref=src, dst_ref=dst, send_sem=ssem, recv_sem=rsem,
            device_id=dev, device_id_type=MESH_IDS,
        )

    def columns(zz):
        return pl.ds(pl.multiple_of(zz * 256, 256), 256)

    barrier = pltpu.get_barrier_semaphore()
    load = local_copy(blocks_hbm, raw, load_sem.at[0])
    load.start()
    load_cols = local_copy(cols_hbm, cols_s, load_sem.at[1])
    load_cols.start()
    greeted = [row_at(z, o) for o in (R, D, L)] + [src_at(z, o) for o in (R, D, L)]
    greeted += [row_at(z1, o) for o in range(4)] + [src_at(z2, 0)]
    odd = lax.rem(z, 2)
    turned = lax.rem(z + 2 * odd + 3, 4)
    crossed = odd * (z // 3) + (1 - odd) * (1 - (z + 3) // 4)
    beyond = (turned, x, y, zh + crossed * (oh - zh), core)
    greeted += [(z, x, y, zh, oc), beyond]
    for dev in greeted:
        pl.semaphore_signal(barrier, inc=1, device_id=dev, device_id_type=MESH_IDS)
    own_moves = [
        local_copy(lists_hbm.at[:, columns(z)], lists_own.at[0, 0], load_sem.at[2]),
        local_copy(lists_hbm.at[:, columns(z2)], lists_own.at[0, 1], load_sem.at[3]),
        local_copy(far_hbm, far_own.at[0], load_sem.at[4]),
    ]
    for move in own_moves:
        move.start()

    zero = jnp.zeros((size, size), jnp.bfloat16)
    for ref, count in ((own, 0), (r_nlr, 2), (r_nd, 1), (r_zo, 1), (r_zlr, 2), (r_zd, 1)):
        for s in range(max(count, 1)):
            if count:
                ref[s, kd] = zero
            else:
                ref[kd] = zero
    for s in range(8):
        accum[s] = jnp.zeros((size, size), jnp.float32)
    load_cols.wait()
    load.wait()
    me = ((z * 4 + x) * 4 + y) * 4 + zh * 2 + core
    rows = lax.broadcasted_iota(jnp.int32, (size, size), 0)
    cols = lax.broadcasted_iota(jnp.int32, (size, size), 1)
    for t in range(kd):
        shift = jnp.where(cols_s[t] == me, 0, size)
        block = raw[t].astype(jnp.float32)
        own[t] = jnp.where(rows + shift > cols, block, 0.0).astype(jnp.bfloat16)

    pl.semaphore_wait(barrier, len(greeted))

    def token(k):
        for dev in (row_at(z1, 0), beyond):
            pl.semaphore_signal(tokens.at[k], inc=1, device_id=dev, device_id_type=MESH_IDS)

    def await_token(k):
        pl.semaphore_wait(tokens.at[k], 2)

    token(0)

    h1, h2 = pl.ds(0, half), pl.ds(half, half)

    def slot_r(o):
        return {R: r_nlr.at[0], L: r_nlr.at[1], D: r_nd.at[0], 4: r_zo.at[0],
                4 + R: r_zlr.at[0], 4 + L: r_zlr.at[1], 4 + D: r_zd.at[0]}[o]

    def slot_q(o):
        return {R: q_nlr.at[0], L: q_nlr.at[1], D: q_nd.at[0], 4: q_zo.at[0],
                4 + R: q_zlr.at[0], 4 + L: q_zlr.at[1], 4 + D: q_zd.at[0]}[o]

    def ring_copies(slot, src, dev, base, ssem, rsem, first_sem, parts, passed):
        right, left = dev(z, 1), dev(z, 3)
        ring, k = {}, first_sem
        for name, o, to in (("L", L, right), ("R", R, left)):
            for p, part in enumerate(parts):
                ring[name + str(p)] = remote(src.at[part], slot(base + o).at[part], ssem.at[k], rsem.at[k], to)
                k += 1
        for p, part in enumerate(parts):
            o, to = (L, right) if passed[p] in "Ll" else (R, left)
            via, to = (slot(base + o), to) if passed[p] in "LR" else (src, dev(z, D))
            ring["D" + str(p)] = remote(via.at[part], slot(base + D).at[part], ssem.at[k], rsem.at[k], to)
            k += 1
        return ring

    halves = (h1, h2)
    quarters = tuple(pl.ds(p * quarter, quarter) for p in range(4))
    rn = ring_copies(slot_r, own, row_at, 0, send_r, recv_r, 0, halves, "LR")
    qn = ring_copies(slot_q, own, src_at, 0, send_q, recv_q, 0, halves, "LR")
    rf = ring_copies(slot_r, slot_r(4), row_at, 4, send_r, recv_r, 6, quarters, "LRlr")
    qf = ring_copies(slot_q, slot_q(4), src_at, 4, send_q, recv_q, 6, quarters, "LRlr")
    rz = [remote(own.at[h], slot_r(4).at[h], send_r.at[18 + k], recv_r.at[18 + k], row_at(z1, 0)) for k, h in enumerate(quarters)]
    qz = [remote(own.at[h], slot_q(4).at[h], send_q.at[18 + k], recv_q.at[18 + k], src_at(z2, 0)) for k, h in enumerate(quarters)]

    middle = (z + 1) // 2 == 1

    def start_outer():
        for copy in rz:
            copy.start()

    pl.when(jnp.logical_not(middle))(start_outer)
    for copy in qz:
        copy.start()
    for ring in (rn, qn):
        ring["L0"].start()
        ring["R1"].start()
    for ring in (rn, qn):
        ring["L1"].start()
        ring["R0"].start()

    list_copies = []
    for o in range(1, 8):
        zz, zt = (z, z2) if o < 4 else (z1, z3)
        dev = row_at(zz, o % 4)
        there = (o // 4) * 4 + back[o % 4]
        list_copies.append(remote(lists_hbm.at[:, columns(zz)], lists_v.at[there, 0], send_l.at[o], recv_l.at[there], dev))
        list_copies.append(remote(lists_hbm.at[:, columns(zt)], lists_v.at[there, 1], send_m.at[o], recv_m.at[there], dev))
        list_copies.append(remote(far_hbm, far_v.at[there], send_f.at[o], recv_f.at[there], dev))
    for copy in list_copies:
        copy.start()

    ub = x + core * (y - x)
    ua = y + core * (x - y)

    def source_place(o):
        b = lax.rem(ub + o, 4)
        xq = b + core * (ua - b)
        yq = ua + core * (b - ua)
        return xq * 4 + yq

    def triples(row_ref, lists, fars, rr, o, acc):
        at_place = source_place(o % 4)
        base = at_place * 16
        far_base = (z if o < 4 else z2) * 64 + at_place * 4
        t = o // 4

        def pick(w):
            left = lists[rr, t, 0, base + w]
            far = fars[rr, 0, far_base + lists[rr, t, 1, base + w]]
            mask = lists[rr, t, 2, base + w]
            left = jnp.where(lists[rr, t, 3, base + w] > 0, left, kd)
            q_ref, q_index = {
                0: (own, None), R: (q_nlr, 0), L: (q_nlr, 1), D: (q_nd, 0), 4: (q_zo, 0),
                4 + R: (q_zlr, 0), 4 + L: (q_zlr, 1), 4 + D: (q_zd, 0),
            }[o]
            far_block = q_ref[far] if q_index is None else q_ref[q_index, far]
            if row_ref is own:
                return own[left], far_block, own[mask]
            at_row = 0 if row_ref is not r_nlr and row_ref is not r_zlr else rr_local
            return row_ref[at_row, left], far_block, row_ref[at_row, mask]

        rr_local = row_local[0]
        for w in range(0, 16, 2):
            l0, f0, m0 = pick(w)
            l1, f1, m1 = pick(w + 1)
            lhs = jnp.concatenate([l0, l1], axis=1)
            rhs = jnp.concatenate(
                [jnp.concatenate([f0, zero], axis=1), jnp.concatenate([zero, f1], axis=1)], axis=0
            )
            product = jnp.dot(lhs, rhs, preferred_element_type=jnp.float32)
            acc = acc + product[:, :size] * m0.astype(jnp.float32)
            acc = acc + product[:, size:] * m1.astype(jnp.float32)
        return acc

    row_local = [0]
    row_groups = {
        "O": (own, lists_own, far_own, (0,), (0,)),
        "LR": (r_nlr, lists_near, far_near, (R, L), (0, 2)),
        "D": (r_nd, lists_near, far_near, (D,), (1,)),
        "zO": (r_zo, lists_far, far_far, (4,), (0,)),
        "zLR": (r_zlr, lists_far, far_far, (4 + R, 4 + L), (1, 3)),
        "zD": (r_zd, lists_far, far_far, (4 + D,), (2,)),
    }
    sources = {"O": (0,), "LR": (R, L), "D": (D,), "zO": (4,), "zLR": (4 + R, 4 + L), "zD": (4 + D,)}

    def work(rgs, qgs):
        for rg in rgs:
            row_ref, lists, fars, slots, at_list = row_groups[rg]

            def one(k, carry):
                row_local[0] = k
                slot = slots[0] if len(slots) == 1 else slots[0] + 2 * k
                rr = at_list[0] if len(slots) == 1 else at_list[0] + 2 * k
                acc = accum[slot]
                for qg in qgs:
                    for o in sources[qg]:
                        acc = triples(row_ref, lists, fars, rr, o, acc)
                accum[slot] = acc
                return carry

            if len(slots) == 1:
                one(0, 0)
            elif sum(len(sources[qg]) for qg in qgs) > 3:
                lax.fori_loop(0, len(slots), one, 0)
            else:
                for k in range(len(slots)):
                    one(k, 0)

    def list_moves(slots):
        moves = []
        for o in slots:
            k, dst_l, dst_f = (o - 1, lists_near, far_near) if o < 4 else (o - 4, lists_far, far_far)
            dev = row_at(z1, 0)
            remote(lists_hbm.at[:, columns(z)], lists_v.at[o, 0], send_l.at[o], recv_l.at[o], dev).wait_recv()
            remote(lists_hbm.at[:, columns(z)], lists_v.at[o, 1], send_m.at[o], recv_m.at[o], dev).wait_recv()
            remote(far_hbm, far_v.at[o], send_f.at[o], recv_f.at[o], dev).wait_recv()
            moves.append(local_copy(lists_v.at[o], dst_l.at[k], smem_sem.at[o]))
            moves.append(local_copy(far_v.at[o], dst_f.at[k], smem_sem.at[8 + o]))
        for move in moves:
            move.start()
        return moves

    def finish(moves):
        for move in moves:
            move.wait()

    def got(ring, *names):
        for name in names:
            ring[name].wait_recv()

    def spread(zcopies, ring, *parts):
        for p in parts:
            zcopies[p].wait_recv()
            ring["L" + str(p)].start()
            ring["R" + str(p)].start()
            if p > 1:
                ring["D" + str(p)].start()

    def relay(ring, *names):
        for name in names:
            ring[name].wait_recv()
            ring["D" + name[1]].start()

    def by_level(run):
        pl.when(middle)(lambda: run(True))
        pl.when(jnp.logical_not(middle))(lambda: run(False))

    near = ["O", "LR", "D"]

    def kinds(mid):
        return ((rz, rf), (qz, qf)) if mid else ((qz, qf), (rz, rf))

    def early(mid, first, others):
        if mid:
            work(first, others)
        else:
            work(others, first)

    def late(mid, second, others):
        early(not mid, second, others)

    def begin(mid):
        if mid:
            for copy in rz:
                copy.start()
        spread(*kinds(mid)[0], 0, 1)

    def turn(mid):
        relay(kinds(mid)[0][1], "L0", "R1")
        spread(*kinds(mid)[1], 0)

    def last(mid):
        (_, ring1), (z_second, ring2) = kinds(mid)
        spread(z_second, ring2, 1)
        finish(list_moves((4, 5, 6, 7)))
        early(mid, ["zO"], near)
        spread(z_second, ring2, 2)
        relay(ring2, "L0")
        got(ring1, "R0", "L1", "L2", "R2", "L3", "R3")
        early(mid, ["zLR"], near)
        spread(z_second, ring2, 3)
        relay(ring2, "R1")
        late(mid, ["zO"], near + ["zO", "zLR"])
        got(ring1, "D0", "D1", "D2", "D3")
        early(mid, ["zD"], near + ["zO"])
        got(ring2, "R0", "L1", "L2", "R2", "L3", "R3")
        late(mid, ["zLR"], near + ["zO", "zLR", "zD"])
        got(ring2, "D0", "D1", "D2", "D3")
        late(mid, ["zD"], near + ["zO", "zLR", "zD"])

    finish(own_moves)
    work(["O"], ["O"])
    relay(rn, "L0", "R1")
    relay(qn, "L0", "R1")
    by_level(begin)
    await_token(0)
    token(1)
    got(rn, "L1", "R0")
    got(qn, "L1", "R0")
    finish(list_moves((1, 2, 3)))
    by_level(lambda mid: spread(*kinds(mid)[0], 2))
    work(["O"], ["LR"])
    by_level(lambda mid: spread(*kinds(mid)[0], 3))
    work(["LR"], ["O", "LR"])
    await_token(1)
    token(2)
    by_level(turn)
    got(rn, "D0", "D1")
    got(qn, "D0", "D1")
    work(["O", "LR"], ["D"])
    work(["D"], near)
    await_token(2)
    token(3)
    by_level(last)
    await_token(3)

    mass = accum[0]
    for s in range(1, 8):
        mass = mass + accum[s]
    whole_sum = jnp.sum(mass, axis=0, keepdims=True)
    part_send[0] = whole_sum
    plane_recv[place] = whole_sum

    def plane_there(k):
        dx, dy = plane[k]
        return plane.index(((4 - dx) % 4, (4 - dy) % 4))

    plane_copies = [
        remote(part_send.at[0], plane_recv.at[place], send_t.at[k], recv_t.at[plane_there(k)], plane_dev(k))
        for k in range(15)
    ]
    for copy in plane_copies:
        copy.start()

    def row_of(s):
        return jnp.sum(jnp.transpose(accum[s]), axis=0, keepdims=True)

    for s in range(1, 8):
        part_send[s] = row_of(s)
    part_copies = []
    for o in range(1, 8):
        dev = row_at(z if o < 4 else z1, o % 4)
        there = (o // 4) * 4 + back[o % 4]
        part_copies.append(remote(part_send.at[o], part_recv.at[there], send_p.at[o], recv_p.at[there], dev))
    for copy in part_copies:
        copy.start()

    for k in range(15):
        remote(part_send.at[0], plane_recv.at[place], send_t.at[k], recv_t.at[k], plane_dev(k)).wait_recv()
    depth_sum = plane_recv[0]
    for p in range(1, 16):
        depth_sum = depth_sum + plane_recv[p]
    depth_send[...] = depth_sum
    depth_recv[level] = depth_sum
    level_copies = [
        remote(depth_send, depth_recv.at[level], send_d.at[k], recv_d.at[k], level_dev(k)) for k in range(15)
    ]
    for copy in level_copies:
        copy.start()
    participation = row_of(0)
    for o in range(1, 8):
        remote(part_send.at[o], part_recv.at[o], send_p.at[o], recv_p.at[o], row_at(z1, 0)).wait_recv()
    for o in range(1, 8):
        participation = participation + part_recv[o]
    part_ref[0:1] = participation

    for ring in (rn, qn, rf, qf):
        for copy in ring.values():
            copy.wait_send()
    for copy in rz + qz + list_copies + part_copies + plane_copies:
        copy.wait_send()
    for copy in level_copies:
        copy.wait_recv()
    grand = depth_recv[0]
    for p in range(1, 16):
        grand = grand + depth_recv[p]
    part_ref[1:2] = jnp.broadcast_to(jnp.sum(grand, axis=1, keepdims=True) * (1.0 / math.sqrt(256 * size)), (1, size))
    for copy in level_copies:
        copy.wait_send()


def local(blocks, block_cols, far_slots, pair_lists):
    kd, size = blocks.shape[0], blocks.shape[1]
    fars = far_slots.shape[1]
    block = (size, size)
    dma = pltpu.SemaphoreType.DMA
    smem = pltpu.SMEM
    vmem = pltpu.VMEM
    bf16, f32, i32 = jnp.bfloat16, jnp.float32, jnp.int32
    result = pl.pallas_call(
        kernel,
        out_shape=jax.ShapeDtypeStruct((2, size), f32),
        in_specs=[pl.BlockSpec(memory_space=pl.ANY)] * 4,
        out_specs=pl.BlockSpec(memory_space=pltpu.VMEM),
        scratch_shapes=[
            vmem((kd,) + block, bf16),
            vmem((kd + 1,) + block, bf16),
            vmem((2, kd + 1) + block, bf16),
            vmem((1, kd + 1) + block, bf16),
            vmem((1, kd + 1) + block, bf16),
            vmem((2, kd + 1) + block, bf16),
            vmem((1, kd + 1) + block, bf16),
            vmem((2, kd) + block, bf16),
            vmem((1, kd) + block, bf16),
            vmem((1, kd) + block, bf16),
            vmem((2, kd) + block, bf16),
            vmem((1, kd) + block, bf16),
            vmem((8, 2, 4, 256), i32),
            vmem((8, 1, fars), i32),
            smem((1, 2, 4, 256), i32),
            smem((1, 1, fars), i32),
            smem((3, 2, 4, 256), i32),
            smem((3, 1, fars), i32),
            smem((4, 2, 4, 256), i32),
            smem((4, 1, fars), i32),
            smem((kd,), i32),
            vmem((8,) + block, f32),
            vmem((8, 1, size), f32),
            vmem((8, 1, size), f32),
            vmem((16, 1, size), f32),
            vmem((1, size), f32),
            vmem((16, 1, size), f32),
            dma((5,)),
            dma((16,)),
            dma((22,)), dma((22,)), dma((22,)), dma((22,)),
            dma((8,)), dma((8,)), dma((8,)), dma((8,)), dma((8,)), dma((8,)),
            dma((8,)), dma((8,)), dma((15,)), dma((15,)), dma((15,)), dma((15,)),
            pltpu.SemaphoreType.REGULAR((4,)),
        ],
        compiler_params=pltpu.CompilerParams(
            collective_id=0, has_side_effects=True, vmem_limit_bytes=60 * 1024 * 1024
        ),
    )(blocks, block_cols, far_slots, pair_lists[0])
    return (result[0], result[1, 0])


def solution(mesh):
    torus = Mesh(mesh.devices.reshape(4, 4, 4, 2, 2), GRP_SUB)
    in_specs = (P(GRP_SUB, None, None), P(GRP_SUB), P(GRP_SUB, None), P(GRP_SUB, None, None))
    out_specs = (P(GRP_SUB), P())
    return jax.shard_map(local, mesh=torus, in_specs=in_specs, out_specs=out_specs, check_vma=False)
```

```python
import functools
import math

import jax
import jax.numpy as jnp
from jax import lax
from jax.experimental import pallas as pl
from jax.experimental.pallas import tpu as pltpu
from jax.sharding import Mesh
from jax.sharding import PartitionSpec as P

GRP = ("grp_0", "grp_1", "grp_2")
SUB = ("sub_0", "sub_1")
GRP_SUB = GRP + SUB
MESH_IDS = pl.DeviceIdType.MESH
R, D, L = 1, 2, 3


def kernel(
    blocks_hbm, cols_hbm, far_hbm, lists_hbm,
    part_ref,
    raw, own, r_nlr, r_nd, r_zo, r_zlr, r_zd, q_nlr, q_nd, q_zo, q_zlr, q_zd,
    lists_v, far_v, lists_own, far_own, lists_near, far_near, lists_far, far_far, cols_s,
    accum, part_send, part_recv, plane_recv, depth_send, depth_recv,
    load_sem, smem_sem,
    send_r, recv_r, send_q, recv_q, send_l, recv_l, send_m, recv_m, send_f, recv_f,
    send_p, recv_p, send_t, recv_t, send_d, recv_d, tokens,
):
    z = lax.axis_index("grp_0")
    x = lax.axis_index("grp_1")
    y = lax.axis_index("grp_2")
    zh = lax.axis_index("sub_0")
    core = lax.axis_index("sub_1")
    kd, size = blocks_hbm.shape[0], blocks_hbm.shape[1]
    half, quarter = kd // 2, kd // 4
    oc, oh = 1 - core, 1 - zh
    z1 = z + 1 - 2 * lax.rem(z, 2)
    z2 = lax.rem(z + 2, 4)
    z3 = 3 - z
    xs = [x] + [lax.rem(x + o, 4) for o in (1, 2, 3)]
    ys = [y] + [lax.rem(y + o, 4) for o in (1, 2, 3)]
    back = (0, L, D, R)

    def row_at(zz, o):
        return (zz, x + core * (xs[o] - x), y + oc * (ys[o] - y), zh, core)

    def src_at(zz, o):
        return (zz, x + oc * (xs[o] - x), y + core * (ys[o] - y), zh, core)

    plane = [(dx, dy) for dx in range(4) for dy in range(4)][1:]
    depth = [(t, c, h) for t in range(4) for c in range(2) for h in range(2)][1:]
    place = x * 4 + y
    level = (zh * 4 + z) * 2 + core

    def plane_dev(k):
        dx, dy = plane[k]
        return (z, xs[dx], ys[dy], zh, core)

    def level_dev(k):
        t, c, h = depth[k]
        return ((z, z1, z2, z3)[t], x, y, (zh, oh)[h], (core, oc)[c])

    def local_copy(src, dst, sem):
        return pltpu.make_async_copy(src, dst, sem)

    def remote(src, dst, ssem, rsem, dev):
        return pltpu.make_async_remote_copy(
            src_ref=src, dst_ref=dst, send_sem=ssem, recv_sem=rsem,
            device_id=dev, device_id_type=MESH_IDS,
        )

    def columns(zz):
        return pl.ds(pl.multiple_of(zz * 256, 256), 256)

    barrier = pltpu.get_barrier_semaphore()
    load = local_copy(blocks_hbm, raw, load_sem.at[0])
    load.start()
    load_cols = local_copy(cols_hbm, cols_s, load_sem.at[1])
    load_cols.start()
    greeted = [row_at(z, o) for o in (R, D, L)] + [src_at(z, o) for o in (R, D, L)]
    greeted += [row_at(z1, o) for o in range(4)] + [src_at(z2, 0)]
    odd = lax.rem(z, 2)
    turned = lax.rem(z + 2 * odd + 3, 4)
    crossed = odd * (z // 3) + (1 - odd) * (1 - (z + 3) // 4)
    beyond = (turned, x, y, zh + crossed * (oh - zh), core)
    greeted += [(z, x, y, zh, oc), beyond]
    for dev in greeted:
        pl.semaphore_signal(barrier, inc=1, device_id=dev, device_id_type=MESH_IDS)
    own_moves = [
        local_copy(lists_hbm.at[:, columns(z)], lists_own.at[0, 0], load_sem.at[2]),
        local_copy(lists_hbm.at[:, columns(z2)], lists_own.at[0, 1], load_sem.at[3]),
        local_copy(far_hbm, far_own.at[0], load_sem.at[4]),
    ]
    for move in own_moves:
        move.start()

    zero = jnp.zeros((size, size), jnp.bfloat16)
    for ref, count in ((own, 0), (r_nlr, 2), (r_nd, 1), (r_zo, 1), (r_zlr, 2), (r_zd, 1)):
        for s in range(max(count, 1)):
            if count:
                ref[s, kd] = zero
            else:
                ref[kd] = zero
    for s in range(8):
        accum[s] = jnp.zeros((size, size), jnp.float32)
    load_cols.wait()
    load.wait()
    me = ((z * 4 + x) * 4 + y) * 4 + zh * 2 + core
    rows = lax.broadcasted_iota(jnp.int32, (size, size), 0)
    cols = lax.broadcasted_iota(jnp.int32, (size, size), 1)
    for t in range(kd):
        shift = jnp.where(cols_s[t] == me, 0, size)
        block = raw[t].astype(jnp.float32)
        own[t] = jnp.where(rows + shift > cols, block, 0.0).astype(jnp.bfloat16)

    pl.semaphore_wait(barrier, len(greeted))

    def token(k):
        for dev in (row_at(z1, 0), beyond):
            pl.semaphore_signal(tokens.at[k], inc=1, device_id=dev, device_id_type=MESH_IDS)

    def await_token(k):
        pl.semaphore_wait(tokens.at[k], 2)

    token(0)

    h1, h2 = pl.ds(0, half), pl.ds(half, half)

    def slot_r(o):
        return {R: r_nlr.at[0], L: r_nlr.at[1], D: r_nd.at[0], 4: r_zo.at[0],
                4 + R: r_zlr.at[0], 4 + L: r_zlr.at[1], 4 + D: r_zd.at[0]}[o]

    def slot_q(o):
        return {R: q_nlr.at[0], L: q_nlr.at[1], D: q_nd.at[0], 4: q_zo.at[0],
                4 + R: q_zlr.at[0], 4 + L: q_zlr.at[1], 4 + D: q_zd.at[0]}[o]

    def ring_copies(slot, src, dev, base, ssem, rsem, first_sem, parts, passed):
        right, left = dev(z, 1), dev(z, 3)
        ring, k = {}, first_sem
        for name, o, to in (("L", L, right), ("R", R, left)):
            for p, part in enumerate(parts):
                ring[name + str(p)] = remote(src.at[part], slot(base + o).at[part], ssem.at[k], rsem.at[k], to)
                k += 1
        for p, part in enumerate(parts):
            o, to = (L, right) if passed[p] in "Ll" else (R, left)
            via, to = (slot(base + o), to) if passed[p] in "LR" else (src, dev(z, D))
            ring["D" + str(p)] = remote(via.at[part], slot(base + D).at[part], ssem.at[k], rsem.at[k], to)
            k += 1
        return ring

    halves = (h1, h2)
    quarters = tuple(pl.ds(p * quarter, quarter) for p in range(4))
    rn = ring_copies(slot_r, own, row_at, 0, send_r, recv_r, 0, halves, "LR")
    qn = ring_copies(slot_q, own, src_at, 0, send_q, recv_q, 0, halves, "LR")
    rf = ring_copies(slot_r, slot_r(4), row_at, 4, send_r, recv_r, 6, quarters, "Lrlr")
    qf = ring_copies(slot_q, slot_q(4), src_at, 4, send_q, recv_q, 6, quarters, "Lrlr")
    rz = [remote(own.at[h], slot_r(4).at[h], send_r.at[18 + k], recv_r.at[18 + k], row_at(z1, 0)) for k, h in enumerate(quarters)]
    qz = [remote(own.at[h], slot_q(4).at[h], send_q.at[18 + k], recv_q.at[18 + k], src_at(z2, 0)) for k, h in enumerate(quarters)]

    middle = (z + 1) // 2 == 1

    def start_outer():
        for copy in rz:
            copy.start()

    pl.when(jnp.logical_not(middle))(start_outer)
    for copy in qz:
        copy.start()
    for ring in (rn, qn):
        ring["L0"].start()
        ring["R1"].start()
    for ring in (rn, qn):
        ring["L1"].start()
        ring["R0"].start()

    list_copies = []
    for o in range(1, 8):
        zz, zt = (z, z2) if o < 4 else (z1, z3)
        dev = row_at(zz, o % 4)
        there = (o // 4) * 4 + back[o % 4]
        list_copies.append(remote(lists_hbm.at[:, columns(zz)], lists_v.at[there, 0], send_l.at[o], recv_l.at[there], dev))
        list_copies.append(remote(lists_hbm.at[:, columns(zt)], lists_v.at[there, 1], send_m.at[o], recv_m.at[there], dev))
        list_copies.append(remote(far_hbm, far_v.at[there], send_f.at[o], recv_f.at[there], dev))
    for copy in list_copies:
        copy.start()

    ub = x + core * (y - x)
    ua = y + core * (x - y)

    def source_place(o):
        b = lax.rem(ub + o, 4)
        xq = b + core * (ua - b)
        yq = ua + core * (b - ua)
        return xq * 4 + yq

    def triples(row_ref, lists, fars, rr, o, acc):
        at_place = source_place(o % 4)
        base = at_place * 16
        far_base = (z if o < 4 else z2) * 64 + at_place * 4
        t = o // 4

        def pick(w):
            left = lists[rr, t, 0, base + w]
            far = fars[rr, 0, far_base + lists[rr, t, 1, base + w]]
            mask = lists[rr, t, 2, base + w]
            left = jnp.where(lists[rr, t, 3, base + w] > 0, left, kd)
            q_ref, q_index = {
                0: (own, None), R: (q_nlr, 0), L: (q_nlr, 1), D: (q_nd, 0), 4: (q_zo, 0),
                4 + R: (q_zlr, 0), 4 + L: (q_zlr, 1), 4 + D: (q_zd, 0),
            }[o]
            far_block = q_ref[far] if q_index is None else q_ref[q_index, far]
            if row_ref is own:
                return own[left], far_block, own[mask]
            at_row = 0 if row_ref is not r_nlr and row_ref is not r_zlr else rr_local
            return row_ref[at_row, left], far_block, row_ref[at_row, mask]

        rr_local = row_local[0]
        for w in range(0, 16, 2):
            l0, f0, m0 = pick(w)
            l1, f1, m1 = pick(w + 1)
            lhs = jnp.concatenate([l0, l1], axis=1)
            rhs = jnp.concatenate(
                [jnp.concatenate([f0, zero], axis=1), jnp.concatenate([zero, f1], axis=1)], axis=0
            )
            product = jnp.dot(lhs, rhs, preferred_element_type=jnp.float32)
            acc = acc + product[:, :size] * m0.astype(jnp.float32)
            acc = acc + product[:, size:] * m1.astype(jnp.float32)
        return acc

    row_local = [0]
    row_groups = {
        "O": (own, lists_own, far_own, (0,), (0,)),
        "LR": (r_nlr, lists_near, far_near, (R, L), (0, 2)),
        "D": (r_nd, lists_near, far_near, (D,), (1,)),
        "zO": (r_zo, lists_far, far_far, (4,), (0,)),
        "zLR": (r_zlr, lists_far, far_far, (4 + R, 4 + L), (1, 3)),
        "zD": (r_zd, lists_far, far_far, (4 + D,), (2,)),
    }
    sources = {"O": (0,), "LR": (R, L), "D": (D,), "zO": (4,), "zLR": (4 + R, 4 + L), "zD": (4 + D,)}

    def work(rgs, qgs):
        for rg in rgs:
            row_ref, lists, fars, slots, at_list = row_groups[rg]

            def one(k, carry):
                row_local[0] = k
                slot = slots[0] if len(slots) == 1 else slots[0] + 2 * k
                rr = at_list[0] if len(slots) == 1 else at_list[0] + 2 * k
                acc = accum[slot]
                for qg in qgs:
                    for o in sources[qg]:
                        acc = triples(row_ref, lists, fars, rr, o, acc)
                accum[slot] = acc
                return carry

            if len(slots) == 1:
                one(0, 0)
            elif sum(len(sources[qg]) for qg in qgs) > 3:
                lax.fori_loop(0, len(slots), one, 0)
            else:
                for k in range(len(slots)):
                    one(k, 0)

    def list_moves(slots):
        moves = []
        for o in slots:
            k, dst_l, dst_f = (o - 1, lists_near, far_near) if o < 4 else (o - 4, lists_far, far_far)
            dev = row_at(z1, 0)
            remote(lists_hbm.at[:, columns(z)], lists_v.at[o, 0], send_l.at[o], recv_l.at[o], dev).wait_recv()
            remote(lists_hbm.at[:, columns(z)], lists_v.at[o, 1], send_m.at[o], recv_m.at[o], dev).wait_recv()
            remote(far_hbm, far_v.at[o], send_f.at[o], recv_f.at[o], dev).wait_recv()
            moves.append(local_copy(lists_v.at[o], dst_l.at[k], smem_sem.at[o]))
            moves.append(local_copy(far_v.at[o], dst_f.at[k], smem_sem.at[8 + o]))
        for move in moves:
            move.start()
        return moves

    def finish(moves):
        for move in moves:
            move.wait()

    def got(ring, *names):
        for name in names:
            ring[name].wait_recv()

    def spread(zcopies, ring, *parts):
        for p in parts:
            zcopies[p].wait_recv()
            ring["L" + str(p)].start()
            ring["R" + str(p)].start()
            if p > 0:
                ring["D" + str(p)].start()

    def relay(ring, *names):
        for name in names:
            ring[name].wait_recv()
            ring["D" + name[1]].start()

    def by_level(run):
        pl.when(middle)(lambda: run(True))
        pl.when(jnp.logical_not(middle))(lambda: run(False))

    near = ["O", "LR", "D"]

    def kinds(mid):
        return ((rz, rf), (qz, qf)) if mid else ((qz, qf), (rz, rf))

    def early(mid, first, others):
        if mid:
            work(first, others)
        else:
            work(others, first)

    def late(mid, second, others):
        early(not mid, second, others)

    def begin(mid):
        if mid:
            for copy in rz:
                copy.start()
        spread(*kinds(mid)[0], 0, 1)

    def turn(mid):
        (relay if True else got)(kinds(mid)[0][1], "L0")
        got(kinds(mid)[0][1], "R1")
        spread(*kinds(mid)[1], 0)

    def last(mid):
        (_, ring1), (z_second, ring2) = kinds(mid)
        spread(z_second, ring2, 1)
        finish(list_moves((4, 5, 6, 7)))
        early(mid, ["zO"], near)
        spread(z_second, ring2, 2)
        relay(ring2, "L0")
        got(ring1, "R0", "L1", "L2", "R2", "L3", "R3")
        early(mid, ["zLR"], near)
        spread(z_second, ring2, 3)
        got(ring2, "R1")
        late(mid, ["zO"], near + ["zO", "zLR"])
        got(ring1, "D0", "D1", "D2", "D3")
        early(mid, ["zD"], near + ["zO"])
        got(ring2, "R0", "L1", "L2", "R2", "L3", "R3")
        late(mid, ["zLR"], near + ["zO", "zLR", "zD"])
        got(ring2, "D0", "D1", "D2", "D3")
        late(mid, ["zD"], near + ["zO", "zLR", "zD"])

    finish(own_moves)
    work(["O"], ["O"])
    relay(rn, "L0", "R1")
    relay(qn, "L0", "R1")
    by_level(begin)
    await_token(0)
    token(1)
    got(rn, "L1", "R0")
    got(qn, "L1", "R0")
    finish(list_moves((1, 2, 3)))
    by_level(lambda mid: spread(*kinds(mid)[0], 2))
    work(["O"], ["LR"])
    by_level(lambda mid: spread(*kinds(mid)[0], 3))
    work(["LR"], ["O", "LR"])
    await_token(1)
    token(2)
    by_level(turn)
    got(rn, "D0", "D1")
    got(qn, "D0", "D1")
    work(["O", "LR"], ["D"])
    work(["D"], near)
    await_token(2)
    token(3)
    by_level(last)
    await_token(3)

    mass = accum[0]
    for s in range(1, 8):
        mass = mass + accum[s]
    whole_sum = jnp.sum(mass, axis=0, keepdims=True)
    part_send[0] = whole_sum
    plane_recv[place] = whole_sum

    def plane_there(k):
        dx, dy = plane[k]
        return plane.index(((4 - dx) % 4, (4 - dy) % 4))

    plane_copies = [
        remote(part_send.at[0], plane_recv.at[place], send_t.at[k], recv_t.at[plane_there(k)], plane_dev(k))
        for k in range(15)
    ]
    for copy in plane_copies:
        copy.start()

    def row_of(s):
        return jnp.sum(jnp.transpose(accum[s]), axis=0, keepdims=True)

    for s in range(1, 8):
        part_send[s] = row_of(s)
    part_copies = []
    for o in range(1, 8):
        dev = row_at(z if o < 4 else z1, o % 4)
        there = (o // 4) * 4 + back[o % 4]
        part_copies.append(remote(part_send.at[o], part_recv.at[there], send_p.at[o], recv_p.at[there], dev))
    for copy in part_copies:
        copy.start()

    for k in range(15):
        remote(part_send.at[0], plane_recv.at[place], send_t.at[k], recv_t.at[k], plane_dev(k)).wait_recv()
    depth_sum = plane_recv[0]
    for p in range(1, 16):
        depth_sum = depth_sum + plane_recv[p]
    depth_send[...] = depth_sum
    depth_recv[level] = depth_sum
    level_copies = [
        remote(depth_send, depth_recv.at[level], send_d.at[k], recv_d.at[k], level_dev(k)) for k in range(15)
    ]
    for copy in level_copies:
        copy.start()
    participation = row_of(0)
    for o in range(1, 8):
        remote(part_send.at[o], part_recv.at[o], send_p.at[o], recv_p.at[o], row_at(z1, 0)).wait_recv()
    for o in range(1, 8):
        participation = participation + part_recv[o]
    part_ref[0:1] = participation

    for ring in (rn, qn, rf, qf):
        for copy in ring.values():
            copy.wait_send()
    for copy in rz + qz + list_copies + part_copies + plane_copies:
        copy.wait_send()
    for copy in level_copies:
        copy.wait_recv()
    grand = depth_recv[0]
    for p in range(1, 16):
        grand = grand + depth_recv[p]
    part_ref[1:2] = jnp.broadcast_to(jnp.sum(grand, axis=1, keepdims=True) * (1.0 / math.sqrt(256 * size)), (1, size))
    for copy in level_copies:
        copy.wait_send()


def local(blocks, block_cols, far_slots, pair_lists):
    kd, size = blocks.shape[0], blocks.shape[1]
    fars = far_slots.shape[1]
    block = (size, size)
    dma = pltpu.SemaphoreType.DMA
    smem = pltpu.SMEM
    vmem = pltpu.VMEM
    bf16, f32, i32 = jnp.bfloat16, jnp.float32, jnp.int32
    result = pl.pallas_call(
        kernel,
        out_shape=jax.ShapeDtypeStruct((2, size), f32),
        in_specs=[pl.BlockSpec(memory_space=pl.ANY)] * 4,
        out_specs=pl.BlockSpec(memory_space=pltpu.VMEM),
        scratch_shapes=[
            vmem((kd,) + block, bf16),
            vmem((kd + 1,) + block, bf16),
            vmem((2, kd + 1) + block, bf16),
            vmem((1, kd + 1) + block, bf16),
            vmem((1, kd + 1) + block, bf16),
            vmem((2, kd + 1) + block, bf16),
            vmem((1, kd + 1) + block, bf16),
            vmem((2, kd) + block, bf16),
            vmem((1, kd) + block, bf16),
            vmem((1, kd) + block, bf16),
            vmem((2, kd) + block, bf16),
            vmem((1, kd) + block, bf16),
            vmem((8, 2, 4, 256), i32),
            vmem((8, 1, fars), i32),
            smem((1, 2, 4, 256), i32),
            smem((1, 1, fars), i32),
            smem((3, 2, 4, 256), i32),
            smem((3, 1, fars), i32),
            smem((4, 2, 4, 256), i32),
            smem((4, 1, fars), i32),
            smem((kd,), i32),
            vmem((8,) + block, f32),
            vmem((8, 1, size), f32),
            vmem((8, 1, size), f32),
            vmem((16, 1, size), f32),
            vmem((1, size), f32),
            vmem((16, 1, size), f32),
            dma((5,)),
            dma((16,)),
            dma((22,)), dma((22,)), dma((22,)), dma((22,)),
            dma((8,)), dma((8,)), dma((8,)), dma((8,)), dma((8,)), dma((8,)),
            dma((8,)), dma((8,)), dma((15,)), dma((15,)), dma((15,)), dma((15,)),
            pltpu.SemaphoreType.REGULAR((4,)),
        ],
        compiler_params=pltpu.CompilerParams(
            collective_id=0, has_side_effects=True, vmem_limit_bytes=60 * 1024 * 1024
        ),
    )(blocks, block_cols, far_slots, pair_lists[0])
    return (result[0], result[1, 0])


def solution(mesh):
    torus = Mesh(mesh.devices.reshape(4, 4, 4, 2, 2), GRP_SUB)
    in_specs = (P(GRP_SUB, None, None), P(GRP_SUB), P(GRP_SUB, None), P(GRP_SUB, None, None))
    out_specs = (P(GRP_SUB), P())
    return jax.shard_map(local, mesh=torus, in_specs=in_specs, out_specs=out_specs, check_vma=False)
```
